256 devices in a mesh: slab: 8 (over z), pencil: 32 (over y, x, core).
Axes of the slice: x: 4, y: 4, z: 8, core: 2. Of those that a mesh axis runs over, the one named last changes fastest.
Arguments:
- right_sides: float32 [8, 128, 128, 128], P(None, 'slab', 'pencil'), may hold values from -6 to 6
- spectrum: float32 [128, 128, 128], P('pencil', 'slab'), may hold values from 0.5 to 20, as said below
- noise_var: float32 [128, 128, 128], P('slab', 'pencil'), may hold values from 0.05 to 1
- observed: int32 [128, 128, 128], P('slab', 'pencil'), may hold values 0 or 1
Outputs:
- solution: float32 [8, 128, 128, 128], P(None, 'slab', 'pencil')
- noise_grad: float32 [128, 128, 128], P('slab', 'pencil')
The draws below stay inside these ranges and needn't reach their ends.
Inputs may be any that keep to these rules, and one draw needn't show every extreme that they name: Even in every index: spectrum[a, b, c] equals spectrum[(-a) mod 128, (-b) mod 128, (-c) mod 128].
All inputs are finite; a program needn't handle non-finite values. No bound on the sum of `observed` on one device may be relied on, other than what follows from the above.
Results may differ from the reference program's by a relative error of at most 0.00021.
Values sent between devices are 32-bit elements; how exact they have to be, the bound alone decides.
A program may use at most 64 MiB of HBM per device.

```python
import math
import jax
import jax.numpy as jnp
from jax import lax

NZ = 128
NY = 128
NX = 128
PROBES = 8
ITERS = 3


def draw_spectrum(key, part):
    base_values = jnp.exp(jax.random.uniform(key, (NX, NY, NZ), jnp.float32, math.log(0.5), math.log(20.0)))
    mirror = jnp.roll(jnp.flip(base_values, (0, 1, 2)), 1, (0, 1, 2))
    return 0.5 * (base_values + mirror)


def touch_ends(array, own_key, low, largest):
    extent = array.shape
    place = [jax.random.randint(jax.random.fold_in(own_key, axis), (), 0, extent[axis]) for axis in range(len(extent))]
    array = array.at[tuple(place)].set(low)
    longest = extent.index(max(extent))
    place[longest] = (place[longest] + 1) % extent[longest]
    return array.at[tuple(place)].set(largest)


def steps_of(own_key, extent, split, low, top_value):
    def one(position, parts):
        draws = jax.random.uniform(jax.random.fold_in(jax.random.fold_in(own_key, 6), position), (parts,), jnp.float32, low / len(split), top_value / len(split))
        return jnp.repeat(jnp.exp(draws), extent[position] // parts).reshape((-1,) + (1,) * (len(extent) - position - 1))

    factor_of = one(*split[0])
    for cut in split[1:]:
        factor_of = factor_of * one(*cut)
    return factor_of


def centred(rng, shape, deviation, reach, split=(), kind=jnp.bfloat16):
    factor_of = steps_of(rng, shape, split, -0.22, 0.18) if split else 1.0
    values = jax.random.normal(rng, shape, jnp.float32) * deviation * factor_of
    return jnp.minimum(jnp.maximum(values, -reach), reach).astype(kind)


def setup_inputs(seed: int = 0) -> dict:
    key_list = jax.random.split(jax.random.key(seed), 5)
    right_sides = centred(key_list[0], (PROBES, NZ, NY, NX), 1.0, 6.0, ((1, 8), (2, 32)), jnp.float32)
    spectrum = draw_spectrum(jax.random.fold_in(key_list[4], 71), 0)
    noise_var = jnp.clip(jnp.exp(math.log(1.0) - 2.9957323 * jax.random.uniform(key_list[2], (NZ, NY, NX), jnp.float32) ** steps_of(key_list[2], (NZ, NY, NX), ((0, 8), (1, 32)), -0.2, 0.2)), 0.05, 1.0)
    observed = touch_ends((jax.random.randint(key_list[3], (NZ, NY, NX), 0, 4) < 3).astype(jnp.int32), jax.random.fold_in(key_list[3], 1), 0, 1)
    return dict(right_sides=right_sides, spectrum=spectrum, noise_var=noise_var, observed=observed)


precise = lax.Precision.HIGHEST

def symmetric(matrix):
    return 0.5 * (matrix + matrix.T)

def solve_spd(matrix, right_hand):
    factor = jnp.linalg.cholesky(symmetric(matrix))
    halfway = lax.linalg.triangular_solve(factor, right_hand, left_side=True, lower=True)
    return lax.linalg.triangular_solve(factor, halfway, left_side=True, lower=True, transpose_a=True)

def gram_local(left, right):
    column_count = left.shape[0]
    return jnp.dot(left.reshape(column_count, -1), right.reshape(column_count, -1).T, precision=precise)

def combine(field_block, coefficients):
    column_count = field_block.shape[0]
    mixed = jnp.dot(coefficients.T, field_block.reshape(column_count, -1), precision=precise)
    return mixed.reshape(field_block.shape)

def operate(field_block, eigen_block, seen_cells, noise_var):
    masked = field_block * seen_cells
    spectral = jnp.fft.fftn(masked, axes=(1, 2, 3))
    smooth = jnp.real(jnp.fft.ifftn(spectral * eigen_block, axes=(1, 2, 3))).astype(jnp.float32)
    return seen_cells * smooth + noise_var * field_block

def reference(right_sides, spectrum, noise_var, observed):
    eigen_block = jnp.transpose(spectrum, (2, 1, 0))
    seen_cells = observed.astype(jnp.float32)
    solution = jnp.zeros_like(right_sides)
    residual = right_sides
    direction = right_sides
    gamma_now = gram_local(residual, residual)
    for iteration in range(ITERS):
        image_block = operate(direction, eigen_block, seen_cells, noise_var)
        delta_now = gram_local(direction, image_block)
        alpha_step = solve_spd(delta_now, gamma_now)
        solution = solution + combine(direction, alpha_step)
        if iteration + 1 < ITERS:
            residual = residual - combine(image_block, alpha_step)
            gamma_next = gram_local(residual, residual)
            beta_step = solve_spd(gamma_now, gamma_next)
            direction = residual + combine(direction, beta_step)
            gamma_now = gamma_next
    weights = right_sides[1:] * solution[1:]
    noise_grad = 0.5 * (solution[0] * solution[0] - jnp.mean(weights, axis=0))
    return (solution, noise_grad)
```

```python
import functools

import jax
import jax.numpy as jnp
import ml_dtypes
import numpy as np
from jax import lax
from jax.experimental import pallas as pl
from jax.experimental.pallas import tpu as pltpu
from jax.sharding import PartitionSpec as P

MESH = pl.DeviceIdType.MESH
F32 = jnp.float32
BF16 = jnp.bfloat16
N = 128
SLAB, PENCIL = 8, 32
INV = 1.0 / (N * N * N)


def split_np(a):
    hi = a.astype(ml_dtypes.bfloat16)
    lo = (a - hi.astype(np.float64)).astype(ml_dtypes.bfloat16)
    return hi, lo


def tables():
    k = np.arange(N)
    ang = 2.0 * np.pi * (np.outer(k, k) % N) / N
    c, s = np.cos(ang), np.sin(ang)
    wx = np.concatenate([c, s], 1)
    place = np.arange(PENCIL * 8)
    a_in, a_out = (-place) % 8, place % 8
    y_in, part_in = 4 * (place // 8) + a_in % 4, a_in // 4
    y_out, part_out = 4 * (place // 8) + a_out % 4, a_out // 4
    wy_f = np.zeros((256, 256))
    wy_i = np.zeros((256, 256))
    for part in range(2):
        for i in range(256):
            wy_f[part * N:(part + 1) * N, i] = (c if part == part_in[i] else (s if part == 0 else -s))[:, y_in[i]]
            wy_i[i, part * N:(part + 1) * N] = (c if part == part_out[i] else (-s if part == 1 else s))[:, y_out[i]]
    wz_f = np.block([[c, -s], [s, c]])
    wz_i = np.block([[c, s], [-s, c]])
    stack = lambda w: np.concatenate(split_np(w), 0)
    return [stack(w) for w in (wx, wy_f, wz_f, wz_i, wy_i)]


def split(v):
    hi = v.astype(BF16)
    return hi, (v - hi.astype(F32)).astype(BF16)


def dot(a, b):
    return lax.dot_general(a, b, (((1,), (0,)), ((), ())), preferred_element_type=F32)


def left_mul(w, v):
    m = w.shape[0] // 2
    hi, lo = split(v)
    t = dot(w[...], hi)
    return t[:m] + (t[m:] + dot(w[:m], lo))


def right_mul(v, w):
    m, k = v.shape
    hi, lo = split(v)
    t = dot(jnp.concatenate([hi, lo], 0), w[:k])
    return t[:m] + (t[m:] + dot(hi, w[k:]))


def iota(shape, axis):
    return lax.broadcasted_iota(jnp.int32, shape, axis)


def chunk_swap(v):
    rows = v.shape[0]
    chunk = iota((rows // 8, 8, 128), 2) // 16
    v = pltpu.roll(v, 0, 1, stride=16, stride_axis=0).reshape(rows // 8, 8, 128)
    for bit in (1, 2, 4):
        v = jnp.where((chunk & bit) != 0, pltpu.roll(v, 8 - bit, 1), v)
    return pltpu.roll(v.reshape(rows, 128), 0, 1, stride=16, stride_axis=0)


def matmul8(a, b):
    out = a[:, 0:1] * b[0:1, :]
    for k in range(1, 8):
        out = out + a[:, k:k + 1] * b[k:k + 1, :]
    return out


def columns_of_transpose(a):
    eye = iota((8, 128), 0) == iota((8, 128), 1)
    return [jnp.sum(jnp.where(eye, a[k:k + 1, :], 0.0), axis=1, keepdims=True) for k in range(8)]


def transpose8(a):
    lane = iota((8, 128), 1)
    out = jnp.zeros((8, 128), F32)
    for k, col in enumerate(columns_of_transpose(a)):
        out = jnp.where(lane == k, col, out)
    return out


def matmul8_tn(a, b):
    cols = columns_of_transpose(a)
    out = cols[0] * b[0:1, :]
    for k in range(1, 8):
        out = out + cols[k] * b[k:k + 1, :]
    return out


def sym8(a):
    return 0.5 * (a + transpose8(a))


def solve8(matrix, rhs):
    row = iota((8, 128), 0)
    aug = jnp.where(iota((8, 128), 1) < 8, sym8(matrix), pltpu.roll(rhs, 8, 1))
    for k in range(8):
        pivot_row = aug[k:k + 1, :] / aug[k:k + 1, k:k + 1]
        aug = jnp.where(row == k, pivot_row, aug - aug[:, k:k + 1] * pivot_row)
    return jnp.where(iota((8, 128), 1) < 8, pltpu.roll(aug, 120, 1), 0.0)


def kernel(rs_ref, spec_ref, noise_ref, seen_ref, wx, wyf, wzf, wzi, wyi, sol_ref, ng_ref,
           r0, u0, w1, w2, r1, ar1, d1, ad1, r2, e, xs, seen, noise, lam, coef,
           sendf, recvf, sendb, recvb, ar_own, ar_plane, ar_mid, ar_slab,
           fs_sem, fr_sem, bs_sem, br_sem, lam_sems, arp_s, arp_r, ars_s, ars_r, enter):
    s = lax.axis_index("slab")
    p = lax.axis_index("pencil")

    barrier = pltpu.get_barrier_semaphore()

    @pl.loop(1, PENCIL)
    def _(o):
        pl.semaphore_signal(barrier, inc=1, device_id=(s, p ^ o), device_id_type=MESH)

    @pl.loop(1, SLAB)
    def _(o):
        pl.semaphore_signal(barrier, inc=1, device_id=((s + o) & 7, p), device_id_type=MESH)

    lane = iota((128, 128), 1)
    sign = jnp.where(lane < 64, 1.0, -1.0).astype(F32)

    for q in range(4):
        rows = [rs_ref[pl.ds((2 * q + c) * 64 + y, 16, stride=4), :] for c in range(2) for y in range(4)]
        r0[q] = jnp.concatenate(rows, 0).T
    rows = [noise_ref[pl.ds(y, 16, stride=4), :] for y in range(4)]
    noise[...] = jnp.concatenate(rows + rows, 0).T
    rows = [seen_ref[pl.ds(y, 16, stride=4), :].astype(F32) for y in range(4)]
    seen[...] = jnp.concatenate(rows + rows, 0).T

    def x_forward(k, h, v):
        mask = seen[...]
        m = jnp.concatenate([v[2 * h] * mask, v[2 * h + 1] * mask], 1)
        sg = jnp.concatenate([sign, sign], 1)
        turned = jnp.concatenate([pltpu.roll(m[:, :128], 64, 1), pltpu.roll(m[:, 128:], 64, 1)], 1) * sg
        out = left_mul(wx, jnp.concatenate([m, turned], 0))
        sendf[k, h, 0:128, :] = out[:, :128]
        sendf[k, h, 128:256, :] = out[:, 128:]

    def x_inverse(k, h, v, out_ref):
        a, b = recvb[k, h, 0:128, :], recvb[k, h, 128:256, :]
        m = jnp.concatenate([a, b], 1)
        sg = jnp.concatenate([sign, sign], 1)
        turned = jnp.concatenate([pltpu.roll(a, 64, 1), pltpu.roll(b, 64, 1)], 1) * (-sg)
        out = left_mul(wx, jnp.concatenate([m, turned], 0))
        for b in range(2):
            out_ref[2 * h + b] = seen[...] * out[:, b * 128:(b + 1) * 128] + noise[...] * v[2 * h + b]

    def middle(k, h):
        t = chunk_swap(recvf[k, h])
        t = left_mul(wyf, t)
        t = right_mul(jnp.concatenate([t[:128], t[128:]], 1), wzf)
        scale = lam[...] * INV
        t = t * jnp.concatenate([scale, scale], 1)
        t = right_mul(t, wzi)
        t = left_mul(wyi, jnp.concatenate([t[:, :128], t[:, 128:]], 0))
        sendb[k, h] = chunk_swap(t)

    def everyone(f):
        for offsets in ((4,), (3, 5), (2, 6), (1, 7), (0,)):
            first = 1 if offsets[0] == 0 else 0

            @pl.loop(first, PENCIL)
            def _(o):
                for so in offsets:
                    f((s + so) & 7, p ^ o)

    plane_row = lambda ts, tp: (ts & 1) * 128 + 4 * tp + (ts >> 1)
    seat_row = lambda ts, tp: tp * 8 + ts
    back_row = lambda ts, tp: tp * 8 + ((8 - ts) & 7)

    def exchange(src, dst, src_row, dst_row, ssem, rsem):
        here = dst_row(s, p)

        def one(ts, tp):
            pltpu.make_async_remote_copy(
                src_ref=src.at[pl.ds(src_row(ts, tp), 1), :], dst_ref=dst.at[pl.ds(here, 1), :],
                send_sem=ssem, recv_sem=rsem, device_id=(ts, tp), device_id_type=MESH).start()
        everyone(one)
        dst[pl.ds(here, 1), :] = src[pl.ds(src_row(s, p), 1), :]

    def wait_rows(ref, n, sem):
        pltpu.make_async_copy(ref.at[pl.ds(0, n), :], ref.at[pl.ds(0, n), :], sem).wait()

    def forward_send(k, h):
        exchange(sendf.at[k, h], recvf.at[k, h], plane_row, seat_row, fs_sem.at[k, h], fr_sem.at[k, h])

    def backward_send(k, h):
        exchange(sendb.at[k, h], recvb.at[k, h], back_row, plane_row, bs_sem.at[k, h], br_sem.at[k, h])

    def gram(u, v, at):
        def step(i, acc):
            rows = pl.ds(pl.multiple_of(i * 8, 8), 8)
            us = [u[q, rows, :] for q in range(4)]
            vs = [v[q, rows, :] for q in range(4)]
            turned = [pltpu.roll(t, 64, 1) for t in vs]
            return tuple(acc[q * 8 + t * 4 + r] + us[q] * (turned if t else vs)[r]
                         for q in range(4) for t in range(2) for r in range(4))
        acc = lax.fori_loop(0, 16, step, tuple(jnp.zeros((8, 128), F32) for _ in range(32)))
        r8, l8 = iota((8, 128), 0), iota((8, 128), 1)
        total = jnp.zeros((1, 128), F32)
        for q in range(4):
            tile = jnp.concatenate([jnp.sum(acc[q * 8 + t], axis=0, keepdims=True) for t in range(8)], 0)
            for c in range(2):
                sums = jnp.sum(jnp.where((l8 // 64) == c, tile, 0.0), axis=1, keepdims=True)
                column = 2 * (r8 & 3) + (c ^ (r8 >> 2))
                hit = l8 == (at - (2 * q + c) * 8) % 128 + column
                total = total + jnp.sum(jnp.where(hit, sums, 0.0), axis=0, keepdims=True)
        return total

    def plane_start(g, row):
        ar_own[g, 0:1, :] = row
        ar_plane[g, pl.ds(p, 1), :] = row

        @pl.loop(1, PENCIL)
        def _(o):
            pltpu.make_async_remote_copy(
                src_ref=ar_own.at[g, pl.ds(0, 1), :], dst_ref=ar_plane.at[g, pl.ds(p, 1), :],
                send_sem=arp_s.at[g], recv_sem=arp_r.at[g], device_id=(s, p ^ o), device_id_type=MESH).start()

    def slab_start(g):
        wait_rows(ar_plane.at[g], PENCIL - 1, arp_r.at[g])
        row = jnp.sum(ar_plane[g], axis=0, keepdims=True)
        ar_mid[g, 0:1, :] = row
        ar_slab[g, pl.ds(s, 1), :] = row
        for o in (4, 3, 5, 2, 6, 1, 7):
            pltpu.make_async_remote_copy(
                src_ref=ar_mid.at[g, pl.ds(0, 1), :], dst_ref=ar_slab.at[g, pl.ds(s, 1), :],
                send_sem=ars_s.at[g], recv_sem=ars_r.at[g], device_id=((s + o) & 7, p), device_id_type=MESH).start()

    def gram_finish(g):
        wait_rows(ar_slab.at[g], SLAB - 1, ars_r.at[g])
        row = jnp.sum(ar_slab[g], axis=0, keepdims=True)
        both = pltpu.roll(jnp.broadcast_to(row, (8, 128)), 0, 1, stride=8, stride_axis=0)
        clean = iota((8, 128), 1) < 8
        return jnp.where(clean, both, 0.0), jnp.where(clean, pltpu.roll(both, 64, 1), 0.0)

    def mix(out, base, terms):
        for slot, (v, small) in enumerate(terms):
            for r in range(4):
                wide = jnp.where(iota((8, 128), 1) < 64, small[:, 2 * r:2 * r + 1], small[:, 2 * r + 1:2 * r + 2])
                low = iota((1, 128), 1) < 64
                for q in range(4):
                    even, odd = wide[2 * q:2 * q + 1, :], wide[2 * q + 1:2 * q + 2, :]
                    coef[slot, r, 2 * q:2 * q + 1, :] = jnp.where(low, even, odd)
                    coef[slot, r, 2 * q + 1:2 * q + 2, :] = jnp.where(low, odd, even)

        @pl.loop(0, 16)
        def _(i):
            rows = pl.ds(pl.multiple_of(i * 8, 8), 8)
            outs = [base[r, rows, :] if base is not None else None for r in range(4)]
            for slot, (v, _small) in enumerate(terms):
                for q in range(4):
                    t = v[q, rows, :]
                    turned = pltpu.roll(t, 64, 1)
                    for r in range(4):
                        add = t * coef[slot, r, 2 * q:2 * q + 1, :] + turned * coef[slot, r, 2 * q + 1:2 * q + 2, :]
                        outs[r] = add if outs[r] is None else outs[r] + add
            for r in range(4):
                out[r, rows, :] = outs[r]

    x_forward(0, 0, r0)
    x_forward(0, 1, r0)

    pl.semaphore_wait(barrier, PENCIL - 1 + SLAB - 1)

    @pl.loop(1, SLAB)
    def _(o):
        pl.semaphore_signal(enter, inc=1, device_id=((s + o) & 7, p), device_id_type=MESH)
    pl.semaphore_wait(enter, SLAB - 1)

    def lam_rows(owner):
        return lam.at[pl.ds(pl.multiple_of(16 * owner, 16), 16), :]

    for o in (4, 3, 5, 2, 6, 1, 7):
        ts = (s + o) & 7
        pltpu.make_async_remote_copy(
            src_ref=spec_ref.at[ts >> 1], dst_ref=lam_rows(s), send_sem=lam_sems.at[0], recv_sem=lam_sems.at[1],
            device_id=(ts, p), device_id_type=MESH).start()
    lam[pl.ds(pl.multiple_of(16 * s, 16), 16), :] = spec_ref[s >> 1]

    forward_send(0, 0)
    forward_send(0, 1)

    def halves(f):
        @pl.loop(0, 2)
        def _(h):
            f(h)

    def middles(k, between=None):
        def one(h):
            wait_rows(recvf.at[k, h], 255, fr_sem.at[k, h])
            middle(k, h)
            backward_send(k, h)
            if between is not None:
                pl.when(h == 0)(between)
        halves(one)

    def inverses(k, v, out, onward):
        def one(h):
            wait_rows(recvb.at[k, h], 255, br_sem.at[k, h])
            x_inverse(k, h, v, out)
            if onward:
                x_forward(k + 1, h, out)
                forward_send(k + 1, h)
        halves(one)

    g00 = gram(r0, r0, 0)
    wait_rows(lam, 112, lam_sems.at[1])
    middles(0)
    inverses(0, r0, u0, True)
    plane_start(0, g00 + gram(r0, u0, 64))
    middles(1, lambda: slab_start(0))
    gamma0, delta0 = gram_finish(0)
    alpha0 = solve8(delta0, gamma0)
    mix(r1, r0, [(u0, -alpha0)])
    mix(xs, None, [(r0, alpha0)])
    g11 = gram(r1, r1, 0)
    inverses(1, u0, w1, True)
    mix(ar1, u0, [(w1, -alpha0)])
    plane_start(1, g11 + gram(r1, ar1, 64))
    middles(2, lambda: slab_start(1))
    gamma1, product1 = gram_finish(1)
    beta0 = solve8(gamma0, gamma1)
    delta1 = product1 - matmul8_tn(beta0, matmul8(delta0, beta0))
    alpha1 = solve8(delta1, gamma1)
    mix(d1, r1, [(r0, beta0)])
    mix(ad1, ar1, [(u0, beta0)])
    mix(r2, r1, [(ad1, -alpha1)])
    mix(e, ar1, [(w1, -(alpha1 + matmul8(beta0, alpha1)))])
    mix(xs, xs, [(d1, alpha1)])
    plane_start(2, gram(r2, r2, 0) + gram(r2, e, 64))
    alpha01 = matmul8(alpha0, alpha1)
    slab_start(2)
    inverses(2, w1, w2, False)
    plane_start(3, gram(r2, w2, 0))
    gamma2, part2 = gram_finish(2)
    beta1 = solve8(gamma1, gamma2)
    older = matmul8_tn(beta1, matmul8(delta1, beta1))
    mix(d1, r2, [(d1, beta1)])
    slab_start(3)
    rest2, _ = gram_finish(3)
    delta2 = sym8(part2 + matmul8(rest2, alpha01)) - older
    alpha2 = solve8(delta2, gamma2)
    mix(xs, xs, [(d1, alpha2)])

    acc = jnp.zeros((128, 128), F32)
    for q in range(4):
        sol = xs[q]
        acc = acc + jnp.where((lane < 64) & (q == 0), 0.0, r0[q] * sol)
        back = sol.T
        for c in range(2):
            for y in range(4):
                sol_ref[pl.ds((2 * q + c) * 64 + y, 16, stride=4), :] = back[c * 64 + y * 16:c * 64 + y * 16 + 16, :]
    mean = (acc + pltpu.roll(acc, 64, 1)) * (1.0 / 7.0)
    back = (0.5 * (xs[0] * xs[0] - mean)).T
    for y in range(4):
        ng_ref[pl.ds(y, 16, stride=4), :] = back[y * 16:y * 16 + 16, :]

    for k in range(3):
        for h in range(2):
            wait_rows(sendf.at[k, h], 255, fs_sem.at[k, h])
            wait_rows(sendb.at[k, h], 255, bs_sem.at[k, h])
    wait_rows(lam, 112, lam_sems.at[0])
    for g in range(4):
        wait_rows(ar_plane.at[g], PENCIL - 1, arp_s.at[g])
        wait_rows(ar_slab.at[g], SLAB - 1, ars_s.at[g])


def local(right_sides, spectrum, noise_var, observed):
    ws = [jnp.asarray(w) for w in tables()]
    block = lambda: pltpu.VMEM((4, 128, 128), F32)
    square = lambda: pltpu.VMEM((128, 128), F32)
    rows = lambda *shape: pltpu.VMEM(shape, F32)
    dma = pltpu.SemaphoreType.DMA
    sol, ng = pl.pallas_call(
        kernel,
        out_shape=(jax.ShapeDtypeStruct((512, 128), F32), jax.ShapeDtypeStruct((64, 128), F32)),
        in_specs=[pl.BlockSpec(memory_space=pltpu.VMEM)] * 9,
        out_specs=[pl.BlockSpec(memory_space=pltpu.VMEM)] * 2,
        scratch_shapes=[block() for _ in range(11)] + [square() for _ in range(3)] + [rows(1, 4, 8, 128)]
        + [rows(3, 2, 256, 128) for _ in range(4)]
        + [rows(4, 8, 128), rows(4, 32, 128), rows(4, 8, 128), rows(4, 8, 128)]
        + [dma((3, 2)) for _ in range(4)] + [dma((2,))] + [dma((4,)) for _ in range(4)]
        + [pltpu.SemaphoreType.REGULAR],
        compiler_params=pltpu.CompilerParams(collective_id=0, has_side_effects=True),
        name="block_cg",
    )(right_sides.reshape(512, 128), spectrum, noise_var.reshape(64, 128), observed.reshape(64, 128), *ws)
    return sol.reshape(8, 16, 4, 128), ng.reshape(16, 4, 128)


def solution(mesh):
    return jax.shard_map(
        local,
        mesh=mesh,
        in_specs=(
            P(None, "slab", "pencil", None),
            P("pencil", "slab", None),
            P("slab", "pencil", None),
            P("slab", "pencil", None),
        ),
        out_specs=(P(None, "slab", "pencil", None), P("slab", "pencil", None)),
        check_vma=False,
    )
```

```python
import functools

import jax
import jax.numpy as jnp
import ml_dtypes
import numpy as np
from jax import lax
from jax.experimental import pallas as pl
from jax.experimental.pallas import tpu as pltpu
from jax.sharding import PartitionSpec as P

MESH = pl.DeviceIdType.MESH
F32 = jnp.float32
BF16 = jnp.bfloat16
N = 128
SLAB, PENCIL = 8, 32
INV = 1.0 / (N * N * N)


def split_np(a):
    hi = a.astype(ml_dtypes.bfloat16)
    lo = (a - hi.astype(np.float64)).astype(ml_dtypes.bfloat16)
    return hi, lo


def tables():
    k = np.arange(N)
    ang = 2.0 * np.pi * (np.outer(k, k) % N) / N
    c, s = np.cos(ang), np.sin(ang)
    kx = 4 * (k % 32) + k // 32
    wx_f = np.concatenate([c[kx], s[kx]], 1)
    wx_i = np.concatenate([c[:, kx], s[:, kx]], 1)
    place = np.arange(PENCIL * 8)
    a_in, a_out = (-place) % 8, place % 8
    y_in, part_in = 4 * (place // 8) + a_in % 4, a_in // 4
    y_out, part_out = 4 * (place // 8) + a_out % 4, a_out // 4
    wy_f = np.zeros((256, 256))
    wy_i = np.zeros((256, 256))
    for part in range(2):
        for i in range(256):
            wy_f[part * N:(part + 1) * N, i] = (c if part == part_in[i] else (s if part == 0 else -s))[:, y_in[i]]
            wy_i[i, part * N:(part + 1) * N] = (c if part == part_out[i] else (-s if part == 1 else s))[:, y_out[i]]
    wz_f = np.block([[c, -s], [s, c]])
    wz_i = np.block([[c, s], [-s, c]])
    stack = lambda w: np.concatenate(split_np(w), 0)
    lane_sum = np.zeros((2, N, N), ml_dtypes.bfloat16)
    place_of = np.zeros((2, 32, N), np.float32)
    for g in range(2):
        for i in range(8):
            for j in range(8):
                lane = (64 * g - 8 * i) % N + j
                lane_sum[g, (i & 1) * 64:(i & 1) * 64 + 64, lane] = 1
                place_of[g, (i >> 1) * 8 + ((i ^ j) & 1) * 4 + (j >> 1), lane] = 1
    return [stack(w) for w in (wx_f, wy_f, wz_f, wz_i, wy_i, wx_i)] + [lane_sum, place_of]


def split(v):
    hi = v.astype(BF16)
    return hi, (v - hi.astype(F32)).astype(BF16)


def dot(a, b):
    return lax.dot_general(a, b, (((1,), (0,)), ((), ())), preferred_element_type=F32)


def left_mul(w, v):
    m = w.shape[0] // 2
    hi, lo = split(v)
    t = dot(w[...], hi)
    return t[:m] + (t[m:] + dot(w[:m], lo))


def right_mul(v, w):
    m, k = v.shape
    hi, lo = split(v)
    t = dot(jnp.concatenate([hi, lo], 0), w[:k])
    return t[:m] + (t[m:] + dot(hi, w[k:]))


def iota(shape, axis):
    return lax.broadcasted_iota(jnp.int32, shape, axis)


def chunk_swap(v):
    rows = v.shape[0]
    chunk = iota((rows // 8, 8, 128), 2) // 16
    v = pltpu.roll(v, 0, 1, stride=16, stride_axis=0).reshape(rows // 8, 8, 128)
    for bit in (1, 2, 4):
        v = jnp.where((chunk & bit) != 0, pltpu.roll(v, 8 - bit, 1), v)
    return pltpu.roll(v.reshape(rows, 128), 0, 1, stride=16, stride_axis=0)


def matmul8(a, b):
    out = a[:, 0:1] * b[0:1, :]
    for k in range(1, 8):
        out = out + a[:, k:k + 1] * b[k:k + 1, :]
    return out


def columns_of_transpose(a):
    eye = iota((8, 128), 0) == iota((8, 128), 1)
    return [jnp.sum(jnp.where(eye, a[k:k + 1, :], 0.0), axis=1, keepdims=True) for k in range(8)]


def transpose8(a):
    lane = iota((8, 128), 1)
    out = jnp.zeros((8, 128), F32)
    for k, col in enumerate(columns_of_transpose(a)):
        out = jnp.where(lane == k, col, out)
    return out


def sym8(a):
    return 0.5 * (a + transpose8(a))


def solve8(matrix, rhs):
    row = iota((8, 128), 0)
    aug = jnp.where(iota((8, 128), 1) < 8, sym8(matrix), pltpu.roll(rhs, 8, 1))
    for k in range(8):
        pivot_row = aug[k:k + 1, :] / aug[k:k + 1, k:k + 1]
        aug = jnp.where(row == k, pivot_row, aug - aug[:, k:k + 1] * pivot_row)
    return jnp.where(iota((8, 128), 1) < 8, pltpu.roll(aug, 120, 1), 0.0)


def kernel(*refs):
    given, (sol_ref, ng_ref), held = refs[:12], refs[12:14], refs[14:26]
    (r0, u0, w1, w2, r1, ar1, d1, r2, e, xs, seen, noise, lam, coef,
     sendf, recvf, sendb, recvb, ar_own, ar_plane, ar_mid, ar_slab, ar_all,
     in_sem, fs_sem, fr_sem, bs_sem, br_sem, lam_sems, arp_s, arp_r, ars_s, ars_r, all_sems, enter) = refs[26:]
    rs_ref, seen_ref, wxf, noise_ref, spec_ref, wyf, wzf, wzi, wyi, wxi, lane_sum, place = held
    loads = [pltpu.make_async_copy(given[i], held[i], in_sem.at[i]) for i in range(12)]
    s = lax.axis_index("slab")
    p = lax.axis_index("pencil")

    barrier = pltpu.get_barrier_semaphore()

    @pl.loop(1, PENCIL)
    def _(o):
        pl.semaphore_signal(barrier, inc=1, device_id=(s, p ^ o), device_id_type=MESH)

    @pl.loop(1, SLAB)
    def _(o):
        pl.semaphore_signal(barrier, inc=1, device_id=((s + o) & 7, p), device_id_type=MESH)

    for load in loads:
        load.start()

    lane = iota((128, 128), 1)
    sign = jnp.where(lane < 64, 1.0, -1.0).astype(F32)

    for load in loads[:4]:
        load.wait()
    for q in range(4):
        rows = [rs_ref[pl.ds((2 * q + c) * 64 + y, 16, stride=4), :] for c in range(2) for y in range(4)]
        r0[q] = jnp.concatenate(rows, 0).T
    rows = [noise_ref[pl.ds(y, 16, stride=4), :] for y in range(4)]
    noise[...] = jnp.concatenate(rows + rows, 0).T
    rows = [seen_ref[pl.ds(y, 16, stride=4), :].astype(F32) for y in range(4)]
    seen[...] = jnp.concatenate(rows + rows, 0).T

    def x_forward(k, h, v):
        mask = seen[...]
        m = jnp.concatenate([v[2 * h] * mask, v[2 * h + 1] * mask], 1)
        sg = jnp.concatenate([sign, sign], 1)
        turned = jnp.concatenate([pltpu.roll(m[:, :128], 64, 1), pltpu.roll(m[:, 128:], 64, 1)], 1) * sg
        out = left_mul(wxf, jnp.concatenate([m, turned], 0))
        for l in range(4):
            for b in range(2):
                sendf[k, h, (2 * l + b) * 32:(2 * l + b) * 32 + 32, :] = out[32 * l:32 * l + 32, b * 128:b * 128 + 128]

    def x_inverse(k, h, v, out_ref):
        a, b = (jnp.concatenate([recvb[k, h, (2 * l + b) * 32:(2 * l + b) * 32 + 32, :] for l in range(4)], 0) for b in range(2))
        m = jnp.concatenate([a, b], 1)
        sg = jnp.concatenate([sign, sign], 1)
        turned = jnp.concatenate([pltpu.roll(a, 64, 1), pltpu.roll(b, 64, 1)], 1) * (-sg)
        out = left_mul(wxi, jnp.concatenate([m, turned], 0))
        for b in range(2):
            out_ref[2 * h + b] = seen[...] * out[:, b * 128:(b + 1) * 128] + noise[...] * v[2 * h + b]

    def middle(k, h):
        t = chunk_swap(recvf[k, h])
        t = left_mul(wyf, t)
        t = right_mul(jnp.concatenate([t[:128], t[128:]], 1), wzf)
        scale = lam[...] * INV
        t = t * jnp.concatenate([scale, scale], 1)
        t = right_mul(t, wzi)
        t = left_mul(wyi, jnp.concatenate([t[:, :128], t[:, 128:]], 0))
        sendb[k, h] = chunk_swap(t)

    def everyone(src, dst, base, chip_step, core_step, ssem, rsem):
        seat, core = p >> 1, p & 1

        def to(chip, c, row):
            pltpu.make_async_remote_copy(
                src_ref=src.at[pl.ds(row, 1), :], dst_ref=dst, send_sem=ssem, recv_sem=rsem,
                device_id=(chip << 1) | c, device_id_type=pl.DeviceIdType.LOGICAL).start()

        def to_chip(chip, row):
            for c in range(2):
                to(chip, c, row + core_step * c)

        for offsets in ((4,), (3, 5), (2, 6), (1, 7)):
            slabs = [(s + so) & 7 for so in offsets]
            pre = [(ts * 16, base(ts)) for ts in slabs]

            @pl.loop(0, 8)
            def _(o):
                for u in range(2):
                    there = seat ^ (2 * o + u)
                    step = chip_step * there
                    for first, row in pre:
                        to_chip(first + there, row + step)

        @pl.loop(1, 16)
        def _(o):
            there = seat ^ o
            to_chip(s * 16 + there, base(s) + chip_step * there)
        to(s * 16 + seat, 1 - core, base(s) + chip_step * seat + core_step * (1 - core))

    def wait_rows(ref, n, sem):
        pltpu.make_async_copy(ref.at[pl.ds(0, n), :], ref.at[pl.ds(0, n), :], sem).wait()

    me = s * 32 + p

    def forward_send(k, h):
        seat_row = p * 8 + s
        everyone(sendf.at[k, h], recvf.at[k, h, pl.ds(seat_row, 1), :], lambda ts: 32 * ts, 2, 1,
                 fs_sem.at[k, h], fr_sem.at[k, h])
        recvf[k, h, pl.ds(seat_row, 1), :] = sendf[k, h, pl.ds(me, 1), :]

    def backward_send(k, h):
        everyone(sendb.at[k, h], recvb.at[k, h, pl.ds(me, 1), :], lambda ts: (8 - ts) & 7, 16, 8,
                 bs_sem.at[k, h], br_sem.at[k, h])
        recvb[k, h, pl.ds(me, 1), :] = sendb[k, h, pl.ds(p * 8 + ((8 - s) & 7), 1), :]

    def gram(u, v, at):
        acc = [None] * 32
        for i in range(16):
            us = [u[q, 8 * i:8 * i + 8, :] for q in range(4)]
            vs = [v[q, 8 * i:8 * i + 8, :] for q in range(4)]
            vs = vs + [pltpu.roll(t, 64, 1) for t in vs]
            for q in range(4):
                for t in range(8):
                    term = us[q] * vs[t]
                    acc[q * 8 + t] = term if i == 0 else acc[q * 8 + t] + term
        tiles = jnp.concatenate(acc, 0)
        hi = tiles.astype(BF16)
        rest = tiles - hi.astype(F32)
        mid = rest.astype(BF16)
        low = (rest - mid.astype(F32)).astype(BF16)
        sums = dot(jnp.concatenate([hi, mid, low], 0), lane_sum[at // 64])
        sums = sums[:256] + (sums[256:512] + sums[512:])
        parts = [sums[8 * t:8 * t + 8] * place[at // 64, t:t + 1, :] for t in range(32)]
        while len(parts) > 1:
            parts = [x + y for x, y in zip(parts[0::2], parts[1::2])]
        return jnp.sum(parts[0], axis=0, keepdims=True)

    def plane_start(g, row):
        ar_own[g, 0:1, :] = row
        ar_plane[g, pl.ds(p, 1), :] = row

        @pl.loop(1, PENCIL)
        def _(o):
            pltpu.make_async_remote_copy(
                src_ref=ar_own.at[g, pl.ds(0, 1), :], dst_ref=ar_plane.at[g, pl.ds(p, 1), :],
                send_sem=arp_s.at[g], recv_sem=arp_r.at[g], device_id=(s, p ^ o), device_id_type=MESH).start()

    def slab_start(g):
        wait_rows(ar_plane.at[g], PENCIL - 1, arp_r.at[g])
        row = jnp.sum(ar_plane[g], axis=0, keepdims=True)
        ar_mid[g, 0:1, :] = row
        ar_slab[g, pl.ds(s, 1), :] = row
        for o in (4, 3, 5, 2, 6, 1, 7):
            pltpu.make_async_remote_copy(
                src_ref=ar_mid.at[g, pl.ds(0, 1), :], dst_ref=ar_slab.at[g, pl.ds(s, 1), :],
                send_sem=ars_s.at[g], recv_sem=ars_r.at[g], device_id=((s + o) & 7, p), device_id_type=MESH).start()

    def gram_finish(g):
        wait_rows(ar_slab.at[g], SLAB - 1, ars_r.at[g])
        return unfold(jnp.sum(ar_slab[g], axis=0, keepdims=True))

    def all_start(row):
        ar_own[2, 0:1, :] = row
        ar_all[pl.ds(me, 1), :] = row
        everyone(ar_own.at[2], ar_all.at[pl.ds(me, 1), :], lambda ts: 0, 0, 0, all_sems.at[0], all_sems.at[1])

    def unfold(row):
        both = pltpu.roll(jnp.broadcast_to(row, (8, 128)), 0, 1, stride=8, stride_axis=0)
        clean = iota((8, 128), 1) < 8
        return jnp.where(clean, both, 0.0), jnp.where(clean, pltpu.roll(both, 64, 1), 0.0)

    def all_finish():
        wait_rows(ar_all, 255, all_sems.at[1])
        tiles = [ar_all[8 * i:8 * i + 8, :] for i in range(32)]
        while len(tiles) > 1:
            tiles = [x + y for x, y in zip(tiles[0::2], tiles[1::2])]
        return unfold(jnp.sum(tiles[0], axis=0, keepdims=True))

    def mix(out, base, terms):
        for slot, (v, small) in enumerate(terms):
            for r in range(4):
                wide = jnp.where(iota((8, 128), 1) < 64, small[:, 2 * r:2 * r + 1], small[:, 2 * r + 1:2 * r + 2])
                low = iota((1, 128), 1) < 64
                for q in range(4):
                    even, odd = wide[2 * q:2 * q + 1, :], wide[2 * q + 1:2 * q + 2, :]
                    coef[slot, r, 2 * q:2 * q + 1, :] = jnp.where(low, even, odd)
                    coef[slot, r, 2 * q + 1:2 * q + 2, :] = jnp.where(low, odd, even)

        for i in range(16):
            rows = slice(8 * i, 8 * i + 8)
            outs = [base[r, rows, :] if base is not None else None for r in range(4)]
            for slot, (v, _small) in enumerate(terms):
                for q in range(4):
                    t = v[q, rows, :]
                    turned = pltpu.roll(t, 64, 1)
                    for r in range(4):
                        add = t * coef[slot, r, 2 * q:2 * q + 1, :] + turned * coef[slot, r, 2 * q + 1:2 * q + 2, :]
                        outs[r] = add if outs[r] is None else outs[r] + add
            for r in range(4):
                out[r, rows, :] = outs[r]

    x_forward(0, 0, r0)
    x_forward(0, 1, r0)
    for load in loads[4:]:
        load.wait()
    g00 = gram(r0, r0, 0)

    pl.semaphore_wait(barrier, PENCIL - 1 + SLAB - 1)

    @pl.loop(1, SLAB)
    def _(o):
        pl.semaphore_signal(enter, inc=1, device_id=((s + o) & 7, p), device_id_type=MESH)
    pl.semaphore_wait(enter, SLAB - 1)

    def lam_rows(owner):
        return lam.at[pl.ds(pl.multiple_of(16 * owner, 16), 16), :]

    for o in (4, 3, 5, 2, 6, 1, 7):
        ts = (s + o) & 7
        pltpu.make_async_remote_copy(
            src_ref=spec_ref.at[ts >> 1], dst_ref=lam_rows(s), send_sem=lam_sems.at[0], recv_sem=lam_sems.at[1],
            device_id=(ts, p), device_id_type=MESH).start()
    lam[pl.ds(pl.multiple_of(16 * s, 16), 16), :] = spec_ref[s >> 1]

    forward_send(0, 0)
    forward_send(0, 1)

    def halves(f):
        @pl.loop(0, 2)
        def _(h):
            f(h)

    def middles(k, between=None):
        def one(h):
            wait_rows(recvf.at[k, h], 255, fr_sem.at[k, h])
            middle(k, h)
            backward_send(k, h)
            if between is not None:
                pl.when(h == 0)(between)
        halves(one)

    def inverses(k, v, out, onward):
        def one(h):
            wait_rows(recvb.at[k, h], 255, br_sem.at[k, h])
            x_inverse(k, h, v, out)
            if onward:
                x_forward(k + 1, h, out)
                forward_send(k + 1, h)
        halves(one)

    wait_rows(lam, 112, lam_sems.at[1])
    middles(0)
    inverses(0, r0, u0, True)
    plane_start(0, g00 + gram(r0, u0, 64))
    eye = jnp.where(iota((8, 128), 0) == iota((8, 128), 1), 1.0, 0.0)
    middles(1, lambda: slab_start(0))
    gamma0, delta0 = gram_finish(0)
    alpha0 = solve8(delta0, gamma0)
    mix(r1, r0, [(u0, -alpha0)])
    g11 = gram(r1, r1, 0)
    inverses(1, u0, w1, True)
    mix(ar1, u0, [(w1, -alpha0)])
    plane_start(1, g11 + gram(r1, ar1, 64))
    inverse0 = solve8(gamma0, eye)
    older0 = matmul8(inverse0, matmul8(delta0, inverse0))
    middles(2, lambda: slab_start(1))
    gamma1, product1 = gram_finish(1)
    beta0 = matmul8(inverse0, gamma1)
    delta1 = product1 - matmul8(gamma1, matmul8(older0, gamma1))
    alpha1 = solve8(delta1, gamma1)
    beta_alpha = matmul8(beta0, alpha1)
    alpha01 = matmul8(alpha0, alpha1)
    mix(r2, r1, [(ar1, -alpha1), (u0, -beta_alpha)])
    mix(e, ar1, [(w1, -(alpha1 + beta_alpha))])
    g22 = gram(r2, r2, 0)
    inverses(2, w1, w2, False)
    mix(e, e, [(w2, alpha01)])
    all_start(g22 + gram(r2, e, 64))
    mix(d1, r1, [(r0, beta0)])
    mix(xs, None, [(r0, alpha0), (d1, alpha1)])
    inverse1 = solve8(gamma1, eye)
    older1 = matmul8(inverse1, matmul8(delta1, inverse1))
    gamma2, product2 = all_finish()
    delta2 = product2 - matmul8(gamma2, matmul8(older1, gamma2))
    alpha2 = solve8(delta2, gamma2)
    mix(xs, xs, [(r2, alpha2), (d1, matmul8(matmul8(inverse1, gamma2), alpha2))])

    acc = jnp.zeros((128, 128), F32)
    for q in range(4):
        sol = xs[q]
        acc = acc + jnp.where((lane < 64) & (q == 0), 0.0, r0[q] * sol)
        back = sol.T
        for c in range(2):
            for y in range(4):
                sol_ref[pl.ds((2 * q + c) * 64 + y, 16, stride=4), :] = back[c * 64 + y * 16:c * 64 + y * 16 + 16, :]
    mean = (acc + pltpu.roll(acc, 64, 1)) * (1.0 / 7.0)
    back = (0.5 * (xs[0] * xs[0] - mean)).T
    for y in range(4):
        ng_ref[pl.ds(y, 16, stride=4), :] = back[y * 16:y * 16 + 16, :]

    for k in range(3):
        for h in range(2):
            wait_rows(sendf.at[k, h], 255, fs_sem.at[k, h])
            wait_rows(sendb.at[k, h], 255, bs_sem.at[k, h])
    wait_rows(lam, 112, lam_sems.at[0])
    wait_rows(ar_all, 255, all_sems.at[0])
    for g in range(2):
        wait_rows(ar_plane.at[g], PENCIL - 1, arp_s.at[g])
        wait_rows(ar_slab.at[g], SLAB - 1, ars_s.at[g])


def local(right_sides, spectrum, noise_var, observed):
    ws = [jnp.asarray(w) for w in tables()]
    block = lambda: pltpu.VMEM((4, 128, 128), F32)
    square = lambda: pltpu.VMEM((128, 128), F32)
    rows = lambda *shape: pltpu.VMEM(shape, F32)
    dma = pltpu.SemaphoreType.DMA
    operands = [right_sides.reshape(512, 128), observed.reshape(64, 128), ws[0], noise_var.reshape(64, 128), spectrum] + ws[1:]
    sol, ng = pl.pallas_call(
        kernel,
        out_shape=(pltpu.VMEM((512, 128), F32), pltpu.VMEM((64, 128), F32)),
        in_specs=[pl.BlockSpec(memory_space=pl.ANY)] * 12,
        out_specs=[pl.BlockSpec(memory_space=pltpu.VMEM)] * 2,
        scratch_shapes=[pltpu.VMEM(a.shape, a.dtype) for a in operands]
        + [block() for _ in range(10)] + [square() for _ in range(3)] + [rows(2, 4, 8, 128)]
        + [rows(3, 2, 256, 128) for _ in range(4)]
        + [rows(3, 8, 128), rows(2, 32, 128), rows(2, 8, 128), rows(2, 8, 128), rows(256, 128)]
        + [dma((12,))] + [dma((3, 2)) for _ in range(4)] + [dma((2,))] + [dma((2,)) for _ in range(4)] + [dma((2,))]
        + [pltpu.SemaphoreType.REGULAR],
        compiler_params=pltpu.CompilerParams(collective_id=0, has_side_effects=True),
        name="block_cg",
    )(*operands)
    return sol.reshape(8, 16, 4, 128), ng.reshape(16, 4, 128)


def solution(mesh):
    return jax.shard_map(
        local,
        mesh=mesh,
        in_specs=(
            P(None, "slab", "pencil", None),
            P("pencil", "slab", None),
            P("slab", "pencil", None),
            P("slab", "pencil", None),
        ),
        out_specs=(P(None, "slab", "pencil", None), P("slab", "pencil", None)),
        check_vma=False,
    )
```

```python
import functools

import jax
import jax.numpy as jnp
import ml_dtypes
import numpy as np
from jax import lax
from jax.experimental import pallas as pl
from jax.experimental.pallas import tpu as pltpu
from jax.sharding import PartitionSpec as P

MESH = pl.DeviceIdType.MESH
F32 = jnp.float32
BF16 = jnp.bfloat16
N = 128
SLAB, PENCIL = 8, 32
HOPS = (0, 1, 2, 1)
FAR_FIRST = sorted(
    [(z, o) for z in range(SLAB) for o in range(16)],
    key=lambda t: (-(min(t[0], SLAB - t[0]) + HOPS[t[1] & 3] + HOPS[t[1] >> 2]), -min(t[0], SLAB - t[0])))
INV = 1.0 / (N * N * N)


def split_np(a):
    hi = a.astype(ml_dtypes.bfloat16)
    lo = (a - hi.astype(np.float64)).astype(ml_dtypes.bfloat16)
    return hi, lo


def tables():
    k = np.arange(N)
    ang = 2.0 * np.pi * (np.outer(k, k) % N) / N
    c, s = np.cos(ang), np.sin(ang)
    kx = 4 * (k % 32) + k // 32
    wx_f = np.concatenate([c[kx], s[kx]], 1)
    wx_i = np.concatenate([c[:, kx], s[:, kx]], 1)
    place = np.arange(PENCIL * 8)
    a_in, a_out = (-place) % 8, place % 8
    y_in, part_in = 4 * (place // 8) + a_in % 4, a_in // 4
    y_out, part_out = 4 * (place // 8) + a_out % 4, a_out // 4
    wy_f = np.zeros((256, 256))
    wy_i = np.zeros((256, 256))
    for part in range(2):
        for i in range(256):
            wy_f[part * N:(part + 1) * N, i] = (c if part == part_in[i] else (s if part == 0 else -s))[:, y_in[i]]
            wy_i[i, part * N:(part + 1) * N] = (c if part == part_out[i] else (-s if part == 1 else s))[:, y_out[i]]
    wz_f = np.block([[c, -s], [s, c]])
    wz_i = np.block([[c, s], [-s, c]])
    stack = lambda w: np.concatenate(split_np(w), 0)
    lane_sum = np.zeros((2, N, N), ml_dtypes.bfloat16)
    place_of = np.zeros((2, 32, N), np.float32)
    for g in range(2):
        for i in range(8):
            for j in range(8):
                lane = (64 * g - 8 * i) % N + j
                lane_sum[g, (i & 1) * 64:(i & 1) * 64 + 64, lane] = 1
                place_of[g, (i >> 1) * 8 + ((i ^ j) & 1) * 4 + (j >> 1), lane] = 1
    return [stack(w) for w in (wx_f, wy_f, wz_f, wz_i, wy_i, wx_i)] + [lane_sum, place_of]


def split(v):
    hi = v.astype(BF16)
    return hi, (v - hi.astype(F32)).astype(BF16)


def dot(a, b):
    return lax.dot_general(a, b, (((1,), (0,)), ((), ())), preferred_element_type=F32)


def left_mul(w, v):
    m = w.shape[0] // 2
    hi, lo = split(v)
    t = dot(w[...], hi)
    return t[:m] + (t[m:] + dot(w[:m], lo))


def right_mul(v, w):
    m, k = v.shape
    hi, lo = split(v)
    t = dot(jnp.concatenate([hi, lo], 0), w[:k])
    return t[:m] + (t[m:] + dot(hi, w[k:]))


def iota(shape, axis):
    return lax.broadcasted_iota(jnp.int32, shape, axis)


def chunk_swap(v):
    rows = v.shape[0]
    chunk = iota((rows // 8, 8, 128), 2) // 16
    v = pltpu.roll(v, 0, 1, stride=16, stride_axis=0).reshape(rows // 8, 8, 128)
    for bit in (1, 2, 4):
        v = jnp.where((chunk & bit) != 0, pltpu.roll(v, 8 - bit, 1), v)
    return pltpu.roll(v.reshape(rows, 128), 0, 1, stride=16, stride_axis=0)


def matmul8(a, b):
    out = a[:, 0:1] * b[0:1, :]
    for k in range(1, 8):
        out = out + a[:, k:k + 1] * b[k:k + 1, :]
    return out


def columns_of_transpose(a):
    eye = iota((8, 128), 0) == iota((8, 128), 1)
    return [jnp.sum(jnp.where(eye, a[k:k + 1, :], 0.0), axis=1, keepdims=True) for k in range(8)]


def transpose8(a):
    lane = iota((8, 128), 1)
    out = jnp.zeros((8, 128), F32)
    for k, col in enumerate(columns_of_transpose(a)):
        out = jnp.where(lane == k, col, out)
    return out


def sym8(a):
    return 0.5 * (a + transpose8(a))


def solve8(matrix, rhs):
    row = iota((8, 128), 0)
    aug = jnp.where(iota((8, 128), 1) < 8, sym8(matrix), pltpu.roll(rhs, 8, 1))
    for k in range(8):
        pivot_row = aug[k:k + 1, :] / aug[k:k + 1, k:k + 1]
        aug = jnp.where(row == k, pivot_row, aug - aug[:, k:k + 1] * pivot_row)
    return jnp.where(iota((8, 128), 1) < 8, pltpu.roll(aug, 120, 1), 0.0)


def kernel(*refs):
    given, (sol_ref, ng_ref), held = refs[:12], refs[12:14], refs[14:26]
    (r0, u0, w1, w2, r1, ar1, d1, r2, e, xs, seen, noise, lam, coef,
     sendf, recvf, sendb, recvb, ar_own, ar_plane, ar_mid, ar_slab, ar_all,
     in_sem, fs_sem, fr_sem, bs_sem, br_sem, lam_sems, arp_s, arp_r, ars_s, ars_r, all_sems, enter) = refs[26:]
    rs_ref, seen_ref, wxf, noise_ref, spec_ref, wyf, wzf, wzi, wyi, wxi, lane_sum, place = held
    loads = [pltpu.make_async_copy(given[i], held[i], in_sem.at[i]) for i in range(12)]
    s = lax.axis_index("slab")
    p = lax.axis_index("pencil")

    barrier = pltpu.get_barrier_semaphore()

    @pl.loop(1, PENCIL)
    def _(o):
        pl.semaphore_signal(barrier, inc=1, device_id=(s, p ^ o), device_id_type=MESH)

    @pl.loop(1, SLAB)
    def _(o):
        pl.semaphore_signal(barrier, inc=1, device_id=((s + o) & 7, p), device_id_type=MESH)

    for load in loads:
        load.start()

    lane = iota((128, 128), 1)
    sign = jnp.where(lane < 64, 1.0, -1.0).astype(F32)

    for load in loads[:4]:
        load.wait()
    for q in range(4):
        rows = [rs_ref[pl.ds((2 * q + c) * 64 + y, 16, stride=4), :] for c in range(2) for y in range(4)]
        r0[q] = jnp.concatenate(rows, 0).T
    rows = [noise_ref[pl.ds(y, 16, stride=4), :] for y in range(4)]
    noise[...] = jnp.concatenate(rows + rows, 0).T
    rows = [seen_ref[pl.ds(y, 16, stride=4), :].astype(F32) for y in range(4)]
    seen[...] = jnp.concatenate(rows + rows, 0).T

    def x_forward(k, h, v):
        mask = seen[...]
        m = jnp.concatenate([v[2 * h] * mask, v[2 * h + 1] * mask], 1)
        sg = jnp.concatenate([sign, sign], 1)
        turned = jnp.concatenate([pltpu.roll(m[:, :128], 64, 1), pltpu.roll(m[:, 128:], 64, 1)], 1) * sg
        out = left_mul(wxf, jnp.concatenate([m, turned], 0))
        for l in range(4):
            for b in range(2):
                sendf[k, h, (2 * l + b) * 32:(2 * l + b) * 32 + 32, :] = out[32 * l:32 * l + 32, b * 128:b * 128 + 128]

    def x_inverse(k, h, v, out_ref):
        a, b = (jnp.concatenate([recvb[k, h, (2 * l + b) * 32:(2 * l + b) * 32 + 32, :] for l in range(4)], 0) for b in range(2))
        m = jnp.concatenate([a, b], 1)
        sg = jnp.concatenate([sign, sign], 1)
        turned = jnp.concatenate([pltpu.roll(a, 64, 1), pltpu.roll(b, 64, 1)], 1) * (-sg)
        out = left_mul(wxi, jnp.concatenate([m, turned], 0))
        for b in range(2):
            out_ref[2 * h + b] = seen[...] * out[:, b * 128:(b + 1) * 128] + noise[...] * v[2 * h + b]

    def middle(k, h):
        t = chunk_swap(recvf[k, h])
        t = left_mul(wyf, t)
        t = right_mul(jnp.concatenate([t[:128], t[128:]], 1), wzf)
        scale = lam[...] * INV
        t = t * jnp.concatenate([scale, scale], 1)
        t = right_mul(t, wzi)
        t = left_mul(wyi, jnp.concatenate([t[:, :128], t[:, 128:]], 0))
        sendb[k, h] = chunk_swap(t)

    def everyone(src, dst, base, chip_step, core_step, ssem, rsem):
        seat, core = p >> 1, p & 1

        def to(chip, c, row):
            pltpu.make_async_remote_copy(
                src_ref=src.at[pl.ds(row, 1), :], dst_ref=dst, send_sem=ssem, recv_sem=rsem,
                device_id=(chip << 1) | c, device_id_type=pl.DeviceIdType.LOGICAL).start()

        def to_chip(chip, row):
            for c in range(2):
                to(chip, c, row + core_step * c)

        slabs = [(s + z) & 7 for z in range(SLAB)]
        pre = [(ts * 16, base(ts)) for ts in slabs]
        for z, o in FAR_FIRST[:-1]:
            there = seat ^ o
            to_chip(pre[z][0] + there, pre[z][1] + chip_step * there)
        to(s * 16 + seat, 1 - core, base(s) + chip_step * seat + core_step * (1 - core))

    def wait_rows(ref, n, sem):
        pltpu.make_async_copy(ref.at[pl.ds(0, n), :], ref.at[pl.ds(0, n), :], sem).wait()

    me = s * 32 + p

    def forward_send(k, h):
        seat_row = p * 8 + s
        everyone(sendf.at[k, h], recvf.at[k, h, pl.ds(seat_row, 1), :], lambda ts: 32 * ts, 2, 1,
                 fs_sem.at[k, h], fr_sem.at[k, h])
        recvf[k, h, pl.ds(seat_row, 1), :] = sendf[k, h, pl.ds(me, 1), :]

    def backward_send(k, h):
        everyone(sendb.at[k, h], recvb.at[k, h, pl.ds(me, 1), :], lambda ts: (8 - ts) & 7, 16, 8,
                 bs_sem.at[k, h], br_sem.at[k, h])
        recvb[k, h, pl.ds(me, 1), :] = sendb[k, h, pl.ds(p * 8 + ((8 - s) & 7), 1), :]

    def gram(u, v, at):
        acc = [None] * 32
        for i in range(16):
            us = [u[q, 8 * i:8 * i + 8, :] for q in range(4)]
            vs = [v[q, 8 * i:8 * i + 8, :] for q in range(4)]
            vs = vs + [pltpu.roll(t, 64, 1) for t in vs]
            for q in range(4):
                for t in range(8):
                    term = us[q] * vs[t]
                    acc[q * 8 + t] = term if i == 0 else acc[q * 8 + t] + term
        tiles = jnp.concatenate(acc, 0)
        hi = tiles.astype(BF16)
        rest = tiles - hi.astype(F32)
        mid = rest.astype(BF16)
        low = (rest - mid.astype(F32)).astype(BF16)
        sums = dot(jnp.concatenate([hi, mid, low], 0), lane_sum[at // 64])
        sums = sums[:256] + (sums[256:512] + sums[512:])
        parts = [sums[8 * t:8 * t + 8] * place[at // 64, t:t + 1, :] for t in range(32)]
        while len(parts) > 1:
            parts = [x + y for x, y in zip(parts[0::2], parts[1::2])]
        return jnp.sum(parts[0], axis=0, keepdims=True)

    def plane_start(g, row):
        ar_own[g, 0:1, :] = row
        ar_plane[g, pl.ds(p, 1), :] = row

        @pl.loop(1, PENCIL)
        def _(o):
            pltpu.make_async_remote_copy(
                src_ref=ar_own.at[g, pl.ds(0, 1), :], dst_ref=ar_plane.at[g, pl.ds(p, 1), :],
                send_sem=arp_s.at[g], recv_sem=arp_r.at[g], device_id=(s, p ^ o), device_id_type=MESH).start()

    def slab_start(g):
        wait_rows(ar_plane.at[g], PENCIL - 1, arp_r.at[g])
        row = jnp.sum(ar_plane[g], axis=0, keepdims=True)
        ar_mid[g, 0:1, :] = row
        ar_slab[g, pl.ds(s, 1), :] = row
        for o in (4, 3, 5, 2, 6, 1, 7):
            pltpu.make_async_remote_copy(
                src_ref=ar_mid.at[g, pl.ds(0, 1), :], dst_ref=ar_slab.at[g, pl.ds(s, 1), :],
                send_sem=ars_s.at[g], recv_sem=ars_r.at[g], device_id=((s + o) & 7, p), device_id_type=MESH).start()

    def gram_finish(g):
        wait_rows(ar_slab.at[g], SLAB - 1, ars_r.at[g])
        return unfold(jnp.sum(ar_slab[g], axis=0, keepdims=True))

    def all_start(row):
        ar_own[2, 0:1, :] = row
        ar_all[pl.ds(me, 1), :] = row
        everyone(ar_own.at[2], ar_all.at[pl.ds(me, 1), :], lambda ts: 0, 0, 0, all_sems.at[0], all_sems.at[1])

    def unfold(row):
        both = pltpu.roll(jnp.broadcast_to(row, (8, 128)), 0, 1, stride=8, stride_axis=0)
        clean = iota((8, 128), 1) < 8
        return jnp.where(clean, both, 0.0), jnp.where(clean, pltpu.roll(both, 64, 1), 0.0)

    def all_finish():
        wait_rows(ar_all, 255, all_sems.at[1])
        tiles = [ar_all[8 * i:8 * i + 8, :] for i in range(32)]
        while len(tiles) > 1:
            tiles = [x + y for x, y in zip(tiles[0::2], tiles[1::2])]
        return unfold(jnp.sum(tiles[0], axis=0, keepdims=True))

    def mix(out, base, terms):
        for slot, (v, small) in enumerate(terms):
            for r in range(4):
                wide = jnp.where(iota((8, 128), 1) < 64, small[:, 2 * r:2 * r + 1], small[:, 2 * r + 1:2 * r + 2])
                low = iota((1, 128), 1) < 64
                for q in range(4):
                    even, odd = wide[2 * q:2 * q + 1, :], wide[2 * q + 1:2 * q + 2, :]
                    coef[slot, r, 2 * q:2 * q + 1, :] = jnp.where(low, even, odd)
                    coef[slot, r, 2 * q + 1:2 * q + 2, :] = jnp.where(low, odd, even)

        for i in range(16):
            rows = slice(8 * i, 8 * i + 8)
            outs = [base[r, rows, :] if base is not None else None for r in range(4)]
            for slot, (v, _small) in enumerate(terms):
                for q in range(4):
                    t = v[q, rows, :]
                    turned = pltpu.roll(t, 64, 1)
                    for r in range(4):
                        add = t * coef[slot, r, 2 * q:2 * q + 1, :] + turned * coef[slot, r, 2 * q + 1:2 * q + 2, :]
                        outs[r] = add if outs[r] is None else outs[r] + add
            for r in range(4):
                out[r, rows, :] = outs[r]

    x_forward(0, 0, r0)
    x_forward(0, 1, r0)
    for load in loads[4:]:
        load.wait()
    g00 = gram(r0, r0, 0)

    pl.semaphore_wait(barrier, PENCIL - 1 + SLAB - 1)

    @pl.loop(1, SLAB)
    def _(o):
        pl.semaphore_signal(enter, inc=1, device_id=((s + o) & 7, p), device_id_type=MESH)

    def lam_rows(owner):
        return lam.at[pl.ds(pl.multiple_of(16 * owner, 16), 16), :]

    for o in (4, 3, 5, 2, 6, 1, 7):
        ts = (s + o) & 7
        pltpu.make_async_remote_copy(
            src_ref=spec_ref.at[ts >> 1], dst_ref=lam_rows(s), send_sem=lam_sems.at[0], recv_sem=lam_sems.at[1],
            device_id=(ts, p), device_id_type=MESH).start()
    lam[pl.ds(pl.multiple_of(16 * s, 16), 16), :] = spec_ref[s >> 1]
    pl.semaphore_wait(enter, SLAB - 1)

    def halves(f):
        @pl.loop(0, 2)
        def _(h):
            f(h)

    halves(lambda h: forward_send(0, h))

    def middles(k, between=None):
        def one(h):
            wait_rows(recvf.at[k, h], 255, fr_sem.at[k, h])
            middle(k, h)
            backward_send(k, h)
            if between is not None:
                pl.when(h == 0)(between)
        halves(one)

    def inverses(k, v, out, onward):
        def one(h):
            wait_rows(recvb.at[k, h], 255, br_sem.at[k, h])
            x_inverse(k, h, v, out)
            if onward:
                x_forward(k + 1, h, out)
                forward_send(k + 1, h)
        halves(one)

    wait_rows(lam, 112, lam_sems.at[1])
    middles(0)
    inverses(0, r0, u0, True)
    plane_start(0, g00 + gram(r0, u0, 64))
    eye = jnp.where(iota((8, 128), 0) == iota((8, 128), 1), 1.0, 0.0)
    middles(1, lambda: slab_start(0))
    gamma0, delta0 = gram_finish(0)
    alpha0 = solve8(delta0, gamma0)
    mix(r1, r0, [(u0, -alpha0)])
    g11 = gram(r1, r1, 0)
    inverses(1, u0, w1, True)
    mix(ar1, u0, [(w1, -alpha0)])
    plane_start(1, g11 + gram(r1, ar1, 64))
    inverse0 = solve8(gamma0, eye)
    older0 = matmul8(inverse0, matmul8(delta0, inverse0))
    middles(2, lambda: slab_start(1))
    gamma1, product1 = gram_finish(1)
    beta0 = matmul8(inverse0, gamma1)
    delta1 = product1 - matmul8(gamma1, matmul8(older0, gamma1))
    alpha1 = solve8(delta1, gamma1)
    beta_alpha = matmul8(beta0, alpha1)
    alpha01 = matmul8(alpha0, alpha1)
    mix(r2, r1, [(ar1, -alpha1), (u0, -beta_alpha)])
    mix(e, ar1, [(w1, -(alpha1 + beta_alpha))])
    g22 = gram(r2, r2, 0)
    inverses(2, w1, w2, False)
    mix(e, e, [(w2, alpha01)])
    all_start(g22 + gram(r2, e, 64))
    mix(d1, r1, [(r0, beta0)])
    mix(xs, None, [(r0, alpha0), (d1, alpha1)])
    inverse1 = solve8(gamma1, eye)
    older1 = matmul8(inverse1, matmul8(delta1, inverse1))
    gamma2, product2 = all_finish()
    delta2 = product2 - matmul8(gamma2, matmul8(older1, gamma2))
    alpha2 = solve8(delta2, gamma2)
    mix(xs, xs, [(r2, alpha2), (d1, matmul8(matmul8(inverse1, gamma2), alpha2))])

    acc = jnp.zeros((128, 128), F32)
    for q in range(4):
        sol = xs[q]
        acc = acc + jnp.where((lane < 64) & (q == 0), 0.0, r0[q] * sol)
        back = sol.T
        for c in range(2):
            for y in range(4):
                sol_ref[pl.ds((2 * q + c) * 64 + y, 16, stride=4), :] = back[c * 64 + y * 16:c * 64 + y * 16 + 16, :]
    mean = (acc + pltpu.roll(acc, 64, 1)) * (1.0 / 7.0)
    back = (0.5 * (xs[0] * xs[0] - mean)).T
    for y in range(4):
        ng_ref[pl.ds(y, 16, stride=4), :] = back[y * 16:y * 16 + 16, :]

    for k in range(3):
        for h in range(2):
            wait_rows(sendf.at[k, h], 255, fs_sem.at[k, h])
            wait_rows(sendb.at[k, h], 255, bs_sem.at[k, h])
    wait_rows(lam, 112, lam_sems.at[0])
    wait_rows(ar_all, 255, all_sems.at[0])
    for g in range(2):
        wait_rows(ar_plane.at[g], PENCIL - 1, arp_s.at[g])
        wait_rows(ar_slab.at[g], SLAB - 1, ars_s.at[g])


def local(right_sides, spectrum, noise_var, observed):
    ws = [jnp.asarray(w) for w in tables()]
    block = lambda: pltpu.VMEM((4, 128, 128), F32)
    square = lambda: pltpu.VMEM((128, 128), F32)
    rows = lambda *shape: pltpu.VMEM(shape, F32)
    dma = pltpu.SemaphoreType.DMA
    operands = [right_sides.reshape(512, 128), observed.reshape(64, 128), ws[0], noise_var.reshape(64, 128), spectrum] + ws[1:]
    sol, ng = pl.pallas_call(
        kernel,
        out_shape=(pltpu.VMEM((512, 128), F32), pltpu.VMEM((64, 128), F32)),
        in_specs=[pl.BlockSpec(memory_space=pl.ANY)] * 12,
        out_specs=[pl.BlockSpec(memory_space=pltpu.VMEM)] * 2,
        scratch_shapes=[pltpu.VMEM(a.shape, a.dtype) for a in operands]
        + [block() for _ in range(10)] + [square() for _ in range(3)] + [rows(2, 4, 8, 128)]
        + [rows(3, 2, 256, 128) for _ in range(4)]
        + [rows(3, 8, 128), rows(2, 32, 128), rows(2, 8, 128), rows(2, 8, 128), rows(256, 128)]
        + [dma((12,))] + [dma((3, 2)) for _ in range(4)] + [dma((2,))] + [dma((2,)) for _ in range(4)] + [dma((2,))]
        + [pltpu.SemaphoreType.REGULAR],
        compiler_params=pltpu.CompilerParams(collective_id=0, has_side_effects=True),
        name="block_cg",
    )(*operands)
    return sol.reshape(8, 16, 4, 128), ng.reshape(16, 4, 128)


def solution(mesh):
    return jax.shard_map(
        local,
        mesh=mesh,
        in_specs=(
            P(None, "slab", "pencil", None),
            P("pencil", "slab", None),
            P("slab", "pencil", None),
            P("slab", "pencil", None),
        ),
        out_specs=(P(None, "slab", "pencil", None), P("slab", "pencil", None)),
        check_vma=False,
    )
```

```python
import functools

import jax
import jax.numpy as jnp
import ml_dtypes
import numpy as np
from jax import lax
from jax.experimental import pallas as pl
from jax.experimental.pallas import tpu as pltpu
from jax.sharding import PartitionSpec as P

MESH = pl.DeviceIdType.MESH
F32 = jnp.float32
BF16 = jnp.bfloat16
N = 128
SLAB, PENCIL = 8, 32
HOPS = (0, 1, 2, 1)
FAR_FIRST = sorted(
    [(z, o) for z in range(SLAB) for o in range(16)],
    key=lambda t: (-(min(t[0], SLAB - t[0]) + HOPS[t[1] & 3] + HOPS[t[1] >> 2]), -min(t[0], SLAB - t[0])))
SEATS = sorted(range(1, PENCIL), key=lambda o: -(HOPS[(o >> 1) & 3] + HOPS[o >> 3]))
INV = 1.0 / (N * N * N)


def split_np(a):
    hi = a.astype(ml_dtypes.bfloat16)
    lo = (a - hi.astype(np.float64)).astype(ml_dtypes.bfloat16)
    return hi, lo


def tables():
    k = np.arange(N)
    ang = 2.0 * np.pi * (np.outer(k, k) % N) / N
    c, s = np.cos(ang), np.sin(ang)
    kx = 4 * (k % 32) + k // 32
    wx_f = np.concatenate([c[kx], s[kx]], 1)
    wx_i = np.concatenate([c[:, kx], s[:, kx]], 1)
    place = np.arange(PENCIL * 8)
    a_in, a_out = (-place) % 8, place % 8
    y_in, part_in = 4 * (place // 8) + a_in % 4, a_in // 4
    y_out, part_out = 4 * (place // 8) + a_out % 4, a_out // 4
    wy_f = np.zeros((256, 256))
    wy_i = np.zeros((256, 256))
    for part in range(2):
        for i in range(256):
            wy_f[part * N:(part + 1) * N, i] = (c if part == part_in[i] else (s if part == 0 else -s))[:, y_in[i]]
            wy_i[i, part * N:(part + 1) * N] = (c if part == part_out[i] else (-s if part == 1 else s))[:, y_out[i]]
    wz_f = np.block([[c, -s], [s, c]])
    wz_i = np.block([[c, s], [-s, c]])
    stack = lambda w: np.concatenate(split_np(w), 0)
    lane_sum = np.zeros((2, N, N), ml_dtypes.bfloat16)
    place_of = np.zeros((2, 32, N), np.float32)
    for g in range(2):
        for i in range(8):
            for j in range(8):
                lane = (64 * g - 8 * i) % N + j
                lane_sum[g, (i & 1) * 64:(i & 1) * 64 + 64, lane] = 1
                place_of[g, (i >> 1) * 8 + ((i ^ j) & 1) * 4 + (j >> 1), lane] = 1
    return [stack(w) for w in (wx_f, wy_f, wz_f, wz_i, wy_i, wx_i)] + [lane_sum, place_of]


def split(v):
    hi = v.astype(BF16)
    return hi, (v - hi.astype(F32)).astype(BF16)


def dot(a, b):
    return lax.dot_general(a, b, (((1,), (0,)), ((), ())), preferred_element_type=F32)


def left_mul(w, v):
    m = w.shape[0] // 2
    hi, lo = split(v)
    t = dot(w[...], hi)
    return t[:m] + (t[m:] + dot(w[:m], lo))


def right_mul(v, w):
    m, k = v.shape
    hi, lo = split(v)
    t = dot(jnp.concatenate([hi, lo], 0), w[:k])
    return t[:m] + (t[m:] + dot(hi, w[k:]))


def iota(shape, axis):
    return lax.broadcasted_iota(jnp.int32, shape, axis)


def chunk_swap(v):
    rows = v.shape[0]
    chunk = iota((rows // 8, 8, 128), 2) // 16
    v = pltpu.roll(v, 0, 1, stride=16, stride_axis=0).reshape(rows // 8, 8, 128)
    for bit in (1, 2, 4):
        v = jnp.where((chunk & bit) != 0, pltpu.roll(v, 8 - bit, 1), v)
    return pltpu.roll(v.reshape(rows, 128), 0, 1, stride=16, stride_axis=0)


def matmul8(a, b):
    out = a[:, 0:1] * b[0:1, :]
    for k in range(1, 8):
        out = out + a[:, k:k + 1] * b[k:k + 1, :]
    return out


def columns_of_transpose(a):
    eye = iota((8, 128), 0) == iota((8, 128), 1)
    return [jnp.sum(jnp.where(eye, a[k:k + 1, :], 0.0), axis=1, keepdims=True) for k in range(8)]


def transpose8(a):
    lane = iota((8, 128), 1)
    out = jnp.zeros((8, 128), F32)
    for k, col in enumerate(columns_of_transpose(a)):
        out = jnp.where(lane == k, col, out)
    return out


def sym8(a):
    return 0.5 * (a + transpose8(a))


def solve8(matrix, rhs):
    row = iota((8, 128), 0)
    aug = jnp.where(iota((8, 128), 1) < 8, sym8(matrix), pltpu.roll(rhs, 8, 1))
    for k in range(8):
        pivot_row = aug[k:k + 1, :] / aug[k:k + 1, k:k + 1]
        aug = jnp.where(row == k, pivot_row, aug - aug[:, k:k + 1] * pivot_row)
    return jnp.where(iota((8, 128), 1) < 8, pltpu.roll(aug, 120, 1), 0.0)


def kernel(*refs):
    given, (sol_ref, ng_ref), held = refs[:12], refs[12:14], refs[14:26]
    (r0, u0, w1, w2, r1, ar1, d1, r2, e, xs, seen, noise, lam, coef,
     sendf, recvf, sendb, recvb, ar_own, ar_plane, ar_mid, ar_slab, ar_all,
     in_sem, fs_sem, fr_sem, bs_sem, br_sem, lam_sems, arp_s, arp_r, ars_s, ars_r, all_sems, enter) = refs[26:]
    rs_ref, seen_ref, wxf, noise_ref, spec_ref, wyf, wzf, wzi, wyi, wxi, lane_sum, place = held
    loads = [pltpu.make_async_copy(given[i], held[i], in_sem.at[i]) for i in range(12)]
    s = lax.axis_index("slab")
    p = lax.axis_index("pencil")

    barrier = pltpu.get_barrier_semaphore()

    for load in loads[:4]:
        load.start()
    for o in (4, 3, 5, 2, 6, 1, 7):
        pl.semaphore_signal(barrier, inc=1, device_id=((s + o) & 7, p), device_id_type=MESH)
    for o in SEATS:
        pl.semaphore_signal(barrier, inc=1, device_id=(s, p ^ o), device_id_type=MESH)

    for load in loads[4:]:
        load.start()

    lane = iota((128, 128), 1)
    sign = jnp.where(lane < 64, 1.0, -1.0).astype(F32)

    for load in loads[:4]:
        load.wait()
    for q in range(4):
        rows = [rs_ref[pl.ds((2 * q + c) * 64 + y, 16, stride=4), :] for c in range(2) for y in range(4)]
        r0[q] = jnp.concatenate(rows, 0).T
    rows = [noise_ref[pl.ds(y, 16, stride=4), :] for y in range(4)]
    noise[...] = jnp.concatenate(rows + rows, 0).T
    rows = [seen_ref[pl.ds(y, 16, stride=4), :].astype(F32) for y in range(4)]
    seen[...] = jnp.concatenate(rows + rows, 0).T

    def x_forward(k, h, v):
        mask = seen[...]
        m = jnp.concatenate([v[2 * h] * mask, v[2 * h + 1] * mask], 1)
        sg = jnp.concatenate([sign, sign], 1)
        turned = jnp.concatenate([pltpu.roll(m[:, :128], 64, 1), pltpu.roll(m[:, 128:], 64, 1)], 1) * sg
        out = left_mul(wxf, jnp.concatenate([m, turned], 0))
        for l in range(4):
            for b in range(2):
                sendf[k, h, (2 * l + b) * 32:(2 * l + b) * 32 + 32, :] = out[32 * l:32 * l + 32, b * 128:b * 128 + 128]

    def x_inverse(k, h, v, out_ref):
        a, b = (jnp.concatenate([recvb[k, h, (2 * l + b) * 32:(2 * l + b) * 32 + 32, :] for l in range(4)], 0) for b in range(2))
        m = jnp.concatenate([a, b], 1)
        sg = jnp.concatenate([sign, sign], 1)
        turned = jnp.concatenate([pltpu.roll(a, 64, 1), pltpu.roll(b, 64, 1)], 1) * (-sg)
        out = left_mul(wxi, jnp.concatenate([m, turned], 0))
        for b in range(2):
            out_ref[2 * h + b] = seen[...] * out[:, b * 128:(b + 1) * 128] + noise[...] * v[2 * h + b]

    def middle(k, h):
        t = chunk_swap(recvf[k, h])
        t = left_mul(wyf, t)
        t = right_mul(jnp.concatenate([t[:128], t[128:]], 1), wzf)
        scale = lam[...] * INV
        t = t * jnp.concatenate([scale, scale], 1)
        t = right_mul(t, wzi)
        t = left_mul(wyi, jnp.concatenate([t[:, :128], t[:, 128:]], 0))
        sendb[k, h] = chunk_swap(t)

    def everyone(src, dst, base, chip_step, core_step, ssem, rsem):
        seat, core = p >> 1, p & 1

        def to(chip, c, row):
            pltpu.make_async_remote_copy(
                src_ref=src.at[pl.ds(row, 1), :], dst_ref=dst, send_sem=ssem, recv_sem=rsem,
                device_id=(chip << 1) | c, device_id_type=pl.DeviceIdType.LOGICAL).start()

        def to_chip(chip, row):
            for c in range(2):
                to(chip, c, row + core_step * c)

        slabs = [(s + z) & 7 for z in range(SLAB)]
        pre = [(ts * 16, base(ts)) for ts in slabs]
        for z, o in FAR_FIRST[:-1]:
            there = seat ^ o
            to_chip(pre[z][0] + there, pre[z][1] + chip_step * there)
        to(s * 16 + seat, 1 - core, base(s) + chip_step * seat + core_step * (1 - core))

    def wait_rows(ref, n, sem):
        pltpu.make_async_copy(ref.at[pl.ds(0, n), :], ref.at[pl.ds(0, n), :], sem).wait()

    me = s * 32 + p

    def forward_send(k, h):
        seat_row = p * 8 + s
        everyone(sendf.at[k, h], recvf.at[k, h, pl.ds(seat_row, 1), :], lambda ts: 32 * ts, 2, 1,
                 fs_sem.at[k, h], fr_sem.at[k, h])
        recvf[k, h, pl.ds(seat_row, 1), :] = sendf[k, h, pl.ds(me, 1), :]

    def backward_send(k, h):
        everyone(sendb.at[k, h], recvb.at[k, h, pl.ds(me, 1), :], lambda ts: (8 - ts) & 7, 16, 8,
                 bs_sem.at[k, h], br_sem.at[k, h])
        recvb[k, h, pl.ds(me, 1), :] = sendb[k, h, pl.ds(p * 8 + ((8 - s) & 7), 1), :]

    def gram(u, v, at):
        acc = [None] * 32
        for i in range(16):
            us = [u[q, 8 * i:8 * i + 8, :] for q in range(4)]
            vs = [v[q, 8 * i:8 * i + 8, :] for q in range(4)]
            vs = vs + [pltpu.roll(t, 64, 1) for t in vs]
            for q in range(4):
                for t in range(8):
                    term = us[q] * vs[t]
                    acc[q * 8 + t] = term if i == 0 else acc[q * 8 + t] + term
        tiles = jnp.concatenate(acc, 0)
        hi = tiles.astype(BF16)
        rest = tiles - hi.astype(F32)
        mid = rest.astype(BF16)
        low = (rest - mid.astype(F32)).astype(BF16)
        sums = dot(jnp.concatenate([hi, mid, low], 0), lane_sum[at // 64])
        sums = sums[:256] + (sums[256:512] + sums[512:])
        parts = [sums[8 * t:8 * t + 8] * place[at // 64, t:t + 1, :] for t in range(32)]
        while len(parts) > 1:
            parts = [x + y for x, y in zip(parts[0::2], parts[1::2])]
        return jnp.sum(parts[0], axis=0, keepdims=True)

    def plane_start(g, row):
        ar_own[g, 0:1, :] = row
        ar_plane[g, pl.ds(p, 1), :] = row

        @pl.loop(1, PENCIL)
        def _(o):
            pltpu.make_async_remote_copy(
                src_ref=ar_own.at[g, pl.ds(0, 1), :], dst_ref=ar_plane.at[g, pl.ds(p, 1), :],
                send_sem=arp_s.at[g], recv_sem=arp_r.at[g], device_id=(s, p ^ o), device_id_type=MESH).start()

    def slab_start(g):
        wait_rows(ar_plane.at[g], PENCIL - 1, arp_r.at[g])
        row = jnp.sum(ar_plane[g], axis=0, keepdims=True)
        ar_mid[g, 0:1, :] = row
        ar_slab[g, pl.ds(s, 1), :] = row
        for o in (4, 3, 5, 2, 6, 1, 7):
            pltpu.make_async_remote_copy(
                src_ref=ar_mid.at[g, pl.ds(0, 1), :], dst_ref=ar_slab.at[g, pl.ds(s, 1), :],
                send_sem=ars_s.at[g], recv_sem=ars_r.at[g], device_id=((s + o) & 7, p), device_id_type=MESH).start()

    def gram_finish(g):
        wait_rows(ar_slab.at[g], SLAB - 1, ars_r.at[g])
        return unfold(jnp.sum(ar_slab[g], axis=0, keepdims=True))

    def all_start(row):
        ar_own[2, 0:1, :] = row
        ar_all[pl.ds(me, 1), :] = row
        everyone(ar_own.at[2], ar_all.at[pl.ds(me, 1), :], lambda ts: 0, 0, 0, all_sems.at[0], all_sems.at[1])

    def unfold(row):
        both = pltpu.roll(jnp.broadcast_to(row, (8, 128)), 0, 1, stride=8, stride_axis=0)
        clean = iota((8, 128), 1) < 8
        return jnp.where(clean, both, 0.0), jnp.where(clean, pltpu.roll(both, 64, 1), 0.0)

    def all_finish():
        wait_rows(ar_all, 255, all_sems.at[1])
        tiles = [ar_all[8 * i:8 * i + 8, :] for i in range(32)]
        while len(tiles) > 1:
            tiles = [x + y for x, y in zip(tiles[0::2], tiles[1::2])]
        return unfold(jnp.sum(tiles[0], axis=0, keepdims=True))

    def mix(out, base, terms):
        for slot, (v, small) in enumerate(terms):
            for r in range(4):
                wide = jnp.where(iota((8, 128), 1) < 64, small[:, 2 * r:2 * r + 1], small[:, 2 * r + 1:2 * r + 2])
                low = iota((1, 128), 1) < 64
                for q in range(4):
                    even, odd = wide[2 * q:2 * q + 1, :], wide[2 * q + 1:2 * q + 2, :]
                    coef[slot, r, 2 * q:2 * q + 1, :] = jnp.where(low, even, odd)
                    coef[slot, r, 2 * q + 1:2 * q + 2, :] = jnp.where(low, odd, even)

        for i in range(16):
            rows = slice(8 * i, 8 * i + 8)
            outs = [base[r, rows, :] if base is not None else None for r in range(4)]
            for slot, (v, _small) in enumerate(terms):
                for q in range(4):
                    t = v[q, rows, :]
                    turned = pltpu.roll(t, 64, 1)
                    for r in range(4):
                        add = t * coef[slot, r, 2 * q:2 * q + 1, :] + turned * coef[slot, r, 2 * q + 1:2 * q + 2, :]
                        outs[r] = add if outs[r] is None else outs[r] + add
            for r in range(4):
                out[r, rows, :] = outs[r]

    x_forward(0, 0, r0)
    x_forward(0, 1, r0)
    for load in loads[4:]:
        load.wait()
    g00 = gram(r0, r0, 0)

    pl.semaphore_wait(barrier, PENCIL - 1 + SLAB - 1)

    for o in (4, 3, 5, 2, 6, 1, 7):
        pl.semaphore_signal(enter, inc=1, device_id=((s + o) & 7, p), device_id_type=MESH)

    def lam_rows(owner):
        return lam.at[pl.ds(pl.multiple_of(16 * owner, 16), 16), :]

    for o in (4, 3, 5, 2, 6, 1, 7):
        ts = (s + o) & 7
        pltpu.make_async_remote_copy(
            src_ref=spec_ref.at[ts >> 1], dst_ref=lam_rows(s), send_sem=lam_sems.at[0], recv_sem=lam_sems.at[1],
            device_id=(ts, p), device_id_type=MESH).start()
    lam[pl.ds(pl.multiple_of(16 * s, 16), 16), :] = spec_ref[s >> 1]
    pl.semaphore_wait(enter, SLAB - 1)

    def halves(f):
        @pl.loop(0, 2)
        def _(h):
            f(h)

    halves(lambda h: forward_send(0, h))

    def middles(k, between=None):
        def one(h):
            wait_rows(recvf.at[k, h], 255, fr_sem.at[k, h])
            middle(k, h)
            backward_send(k, h)
            if between is not None:
                pl.when(h == 0)(between)
        halves(one)

    def inverses(k, v, out, onward):
        def one(h):
            wait_rows(recvb.at[k, h], 255, br_sem.at[k, h])
            x_inverse(k, h, v, out)
            if onward:
                x_forward(k + 1, h, out)
                forward_send(k + 1, h)
        halves(one)

    wait_rows(lam, 112, lam_sems.at[1])
    middles(0)
    inverses(0, r0, u0, True)
    plane_start(0, g00 + gram(r0, u0, 64))
    eye = jnp.where(iota((8, 128), 0) == iota((8, 128), 1), 1.0, 0.0)
    middles(1, lambda: slab_start(0))
    gamma0, delta0 = gram_finish(0)
    alpha0 = solve8(delta0, gamma0)
    mix(r1, r0, [(u0, -alpha0)])
    g11 = gram(r1, r1, 0)
    inverses(1, u0, w1, True)
    mix(ar1, u0, [(w1, -alpha0)])
    plane_start(1, g11 + gram(r1, ar1, 64))
    inverse0 = solve8(gamma0, eye)
    older0 = matmul8(inverse0, matmul8(delta0, inverse0))
    middles(2, lambda: slab_start(1))
    gamma1, product1 = gram_finish(1)
    beta0 = matmul8(inverse0, gamma1)
    delta1 = product1 - matmul8(gamma1, matmul8(older0, gamma1))
    alpha1 = solve8(delta1, gamma1)
    beta_alpha = matmul8(beta0, alpha1)
    alpha01 = matmul8(alpha0, alpha1)
    mix(r2, r1, [(ar1, -alpha1), (u0, -beta_alpha)])
    mix(e, ar1, [(w1, -(alpha1 + beta_alpha))])
    g22 = gram(r2, r2, 0)
    inverses(2, w1, w2, False)
    mix(e, e, [(w2, alpha01)])
    all_start(g22 + gram(r2, e, 64))
    mix(d1, r1, [(r0, beta0)])
    mix(xs, None, [(r0, alpha0), (d1, alpha1)])
    inverse1 = solve8(gamma1, eye)
    older1 = matmul8(inverse1, matmul8(delta1, inverse1))
    gamma2, product2 = all_finish()
    delta2 = product2 - matmul8(gamma2, matmul8(older1, gamma2))
    alpha2 = solve8(delta2, gamma2)
    mix(xs, xs, [(r2, alpha2), (d1, matmul8(matmul8(inverse1, gamma2), alpha2))])

    acc = jnp.zeros((128, 128), F32)
    for q in range(4):
        sol = xs[q]
        acc = acc + jnp.where((lane < 64) & (q == 0), 0.0, r0[q] * sol)
        back = sol.T
        for c in range(2):
            for y in range(4):
                sol_ref[pl.ds((2 * q + c) * 64 + y, 16, stride=4), :] = back[c * 64 + y * 16:c * 64 + y * 16 + 16, :]
    mean = (acc + pltpu.roll(acc, 64, 1)) * (1.0 / 7.0)
    back = (0.5 * (xs[0] * xs[0] - mean)).T
    for y in range(4):
        ng_ref[pl.ds(y, 16, stride=4), :] = back[y * 16:y * 16 + 16, :]

    for k in range(3):
        for h in range(2):
            wait_rows(sendf.at[k, h], 255, fs_sem.at[k, h])
            wait_rows(sendb.at[k, h], 255, bs_sem.at[k, h])
    wait_rows(lam, 112, lam_sems.at[0])
    wait_rows(ar_all, 255, all_sems.at[0])
    for g in range(2):
        wait_rows(ar_plane.at[g], PENCIL - 1, arp_s.at[g])
        wait_rows(ar_slab.at[g], SLAB - 1, ars_s.at[g])


def local(right_sides, spectrum, noise_var, observed):
    ws = [jnp.asarray(w) for w in tables()]
    block = lambda: pltpu.VMEM((4, 128, 128), F32)
    square = lambda: pltpu.VMEM((128, 128), F32)
    rows = lambda *shape: pltpu.VMEM(shape, F32)
    dma = pltpu.SemaphoreType.DMA
    operands = [right_sides.reshape(512, 128), observed.reshape(64, 128), ws[0], noise_var.reshape(64, 128), spectrum] + ws[1:]
    sol, ng = pl.pallas_call(
        kernel,
        out_shape=(pltpu.VMEM((512, 128), F32), pltpu.VMEM((64, 128), F32)),
        in_specs=[pl.BlockSpec(memory_space=pl.ANY)] * 12,
        out_specs=[pl.BlockSpec(memory_space=pltpu.VMEM)] * 2,
        scratch_shapes=[pltpu.VMEM(a.shape, a.dtype) for a in operands]
        + [block() for _ in range(10)] + [square() for _ in range(3)] + [rows(2, 4, 8, 128)]
        + [rows(3, 2, 256, 128) for _ in range(4)]
        + [rows(3, 8, 128), rows(2, 32, 128), rows(2, 8, 128), rows(2, 8, 128), rows(256, 128)]
        + [dma((12,))] + [dma((3, 2)) for _ in range(4)] + [dma((2,))] + [dma((2,)) for _ in range(4)] + [dma((2,))]
        + [pltpu.SemaphoreType.REGULAR],
        compiler_params=pltpu.CompilerParams(collective_id=0, has_side_effects=True),
        name="block_cg",
    )(*operands)
    return sol.reshape(8, 16, 4, 128), ng.reshape(16, 4, 128)


def solution(mesh):
    return jax.shard_map(
        local,
        mesh=mesh,
        in_specs=(
            P(None, "slab", "pencil", None),
            P("pencil", "slab", None),
            P("slab", "pencil", None),
            P("slab", "pencil", None),
        ),
        out_specs=(P(None, "slab", "pencil", None), P("slab", "pencil", None)),
        check_vma=False,
    )
```
